256 devices in a mesh: row: 8 (over z), col: 8 (over x_lo, y), layer: 4 (over x_hi, core).
Axes of the slice: x: 4 (x_hi: 2, x_lo: 2; x = x_hi * 2 + x_lo), y: 4, z: 8, core: 2. Of those that a mesh axis runs over, the one named last changes fastest.
Arguments:
- tokens: bfloat16 [5120, 6144], P('row', 'layer'), may hold values from -6 to 6
- expert_ids: int32 [5120, 2], replicated, may hold values from 0 to 7, all different within a row; in each aligned block of 5120 rows (0 to 5119, 5120 to 10239, ...) at most 2560 rows name the same one
- w_gate: bfloat16 [2, 6144, 8192], P(None, 'layer', ('row', 'col')), may hold values from -0.078125 to 0.078125
- w_up: bfloat16 [2, 6144, 8192], P(None, 'layer', ('row', 'col')), may hold values from -0.078125 to 0.078125
Outputs:
- hidden: bfloat16 [2, 2560, 8192], P(None, ('col', 'layer'), 'row')
The draws below stay inside these ranges and needn't reach their ends.
Inputs may be any that keep to these rules, and one draw needn't show every extreme that they name: `expert_ids`: each token names 2 different experts. No expert is named by more than 2560 tokens, a bound that some block reaches.
All inputs are finite; a program needn't handle non-finite values.
Results may differ from the reference program's by a relative error of at most 0.0012.
Values may be sent and summed in bfloat16 or wider, within the bound.
No kernel may reach another device: no remote copies, remote signals or barrier semaphores. Data moves between devices by JAX's collectives and lax.ppermute only.
A program may use at most 128 MiB of HBM per device.

```python
import math
import jax
import jax.numpy as jnp
import numpy as np

D = 6144
EXPERTS = 8
TOP = 2
FF = 8192
EXP_FLIGHT = 2
SLOTS_DEV = 80
CAP = 2560
TOKENS = 5120
N_COL = 8
N_LAYER = 4


def block_scale(stream_key, extent, shards, low, top_value):
    def one(axis_at, shards_of):
        heights = jax.random.uniform(jax.random.fold_in(jax.random.fold_in(stream_key, 6), axis_at), (shards_of,), jnp.float32, low / len(shards), top_value / len(shards))
        return jnp.repeat(jnp.exp(heights), extent[axis_at] // shards_of).reshape((-1,) + (1,) * (len(extent) - axis_at - 1))

    factor_of = one(*shards[0])
    for cut in shards[1:]:
        factor_of = factor_of * one(*cut)
    return factor_of


def deal_out(rng, own, number, rows, number_of, top, most, slope):
    order = jax.random.permutation(rng, number_of)
    heavy_load, ordinary = load_shares(number_of, rows * top, most, slope, True), load_shares(number_of, rows * top, most, slope, False)
    places = jnp.arange(number_of)

    def named(lengths, offset_by):
        used = int((lengths > 0).sum())
        fixed = max(1, used // 4)
        passed = fixed + (places - fixed + offset_by * (used - fixed)) % max(1, number_of - fixed)
        return jnp.zeros((number_of,), jnp.int32).at[order[jnp.where(places < fixed, places, passed)]].set(jnp.asarray(lengths, jnp.int32))

    lengths = jnp.where(number % 4 == 0, named(heavy_load, number // 4), named(ordinary, number - number // 4 - 1))
    mixed = jax.random.permutation(jax.random.fold_in(own, 3), number_of)
    giver, receiver = mixed[0:number_of // 2 * 2:2], mixed[1:number_of // 2 * 2:2]
    room = jnp.minimum(lengths[giver] - 1, most - lengths[receiver]) // 2
    room = jnp.where((giver == order[0]) | (receiver == order[0]) | (lengths[receiver] == 0), 0, jnp.maximum(room, 0))
    passed = jax.random.randint(jax.random.fold_in(own, 4), (number_of // 2,), 0, 1 << 20) % (room + 1)
    lengths = lengths.at[giver].add(-passed).at[receiver].add(passed)
    members = jnp.searchsorted(jnp.cumsum(lengths), jnp.arange(rows * top), side="right").astype(jnp.int32)
    listing = members.reshape(top, rows).T
    listing = listing[jax.random.permutation(jax.random.fold_in(own, 1), rows)]
    offset_by = jax.random.randint(jax.random.fold_in(own, 2), (rows, 1), 0, top)
    return jnp.take_along_axis(listing, (jnp.arange(top)[None, :] + offset_by) % top, axis=1)


def load_shares(number_of, total, reach, slope, full):
    weights = [(1 << 20) // math.isqrt(standing ** slope) + 1 for standing in range(1, number_of + 1)]
    largest = reach if full else min(reach, max(-(-total // number_of), total * weights[0] // sum(weights)))
    least = 1 if total - largest >= number_of - 1 else 0
    given, surplus = [largest] + [least] * (number_of - 1), total - largest - least * (number_of - 1)
    while surplus > 0:
        candidates = [i for i in range(1, number_of) if given[i] < largest] or [i for i in range(1, number_of) if given[i] < reach]
        whole, remaining = sum([weights[i] for i in candidates]), surplus
        for i in candidates:
            addition = min(reach - given[i], max(1, remaining * weights[i] // whole), surplus)
            given[i] = given[i] + addition
            surplus = surplus - addition
    return np.array(given)


def centred(key, dims, scale, limit, shards=(), kind=jnp.bfloat16):
    loudness = block_scale(key, dims, shards, -0.22, 0.18) if shards else 1.0
    entries = jax.random.normal(key, dims, jnp.float32) * scale * loudness
    return jnp.minimum(jnp.maximum(entries, -limit), limit).astype(kind)


def setup_inputs(seed: int = 0) -> dict:
    streams_of = jax.random.split(jax.random.key(seed), 5)
    tokens = centred(streams_of[0], (TOKENS, D), 1.0, 6.0, ((0, 8), (1, 4)))
    expert_ids_keys = jax.random.split(jax.random.fold_in(streams_of[1], 1), TOKENS // TOKENS)
    expert_ids_turns = jax.random.permutation(jax.random.fold_in(streams_of[1], 3), TOKENS // TOKENS)
    expert_ids = jax.vmap(lambda own, number: deal_out(jax.random.fold_in(streams_of[1], 2), own, number, TOKENS, EXPERTS, TOP, CAP, 2))(expert_ids_keys, expert_ids_turns).reshape((TOKENS, TOP))
    w_gate = centred(streams_of[2], (EXP_FLIGHT, D, FF), D ** -0.5, 0.078125, ((1, 4), (2, 64)))
    w_up = centred(streams_of[3], (EXP_FLIGHT, D, FF), D ** -0.5, 0.078125, ((1, 4), (2, 64)))
    return {"tokens": tokens, "expert_ids": expert_ids, "w_gate": w_gate, "w_up": w_up}


def reference(tokens, expert_ids, w_gate, w_up):
    tok_count = tokens.shape[0]
    capacity = SLOTS_DEV * N_COL * N_LAYER
    expert_range = jnp.arange(EXP_FLIGHT, dtype=jnp.int32)
    member = jnp.any(expert_ids[:, :, None] == expert_range[None, None, :], axis=1).astype(jnp.int32)
    slot_rank = (jnp.cumsum(member, axis=0) - member).astype(jnp.int32)
    target = jnp.where(member > 0, slot_rank, capacity).astype(jnp.int32)
    token_range = jnp.broadcast_to(jnp.arange(tok_count, dtype=jnp.int32)[:, None], target.shape)
    slot_table = jnp.zeros((EXP_FLIGHT, capacity + 1), jnp.int32).at[expert_range[None, :], target].set(token_range)
    counts = jnp.sum(member, axis=0).astype(jnp.int32)
    live_mask = jnp.arange(capacity, dtype=jnp.int32)[None, :] < counts[:, None]
    results = []
    for expert in range(EXP_FLIGHT):
        slot_rows = jnp.where(live_mask[expert][:, None], tokens[slot_table[expert, :capacity]], jnp.zeros((), tokens.dtype))
        gate = jnp.dot(slot_rows, w_gate[expert], preferred_element_type=jnp.float32)
        up_part = jnp.dot(slot_rows, w_up[expert], preferred_element_type=jnp.float32)
        results.append((jax.nn.silu(gate) * up_part).astype(jnp.bfloat16))
    return jnp.stack(results)
```

```python
import jax
import jax.numpy as jnp
from jax import lax
from jax.sharding import PartitionSpec as P


ROWS = 8
SETS = 4
HALVES = 2
QUARTERS = 4
SLOTS_DEV = 80
SEND = 168
DEAL = 21
GROUP = HALVES * SETS * DEAL


def y_perm(step):
    return [
        (h * SETS + s, h * SETS + (s + step) % SETS) for h in range(HALVES) for s in range(SETS)
    ]


def z_perm(step):
    return [(z, (z + step) % ROWS) for z in range(ROWS)]


def layer_perm(bit):
    return [(q, q ^ bit) for q in range(QUARTERS)]


def below(n, s):
    return (n + (SETS - 1) - s) >> 2


def weights_of_ring(w_gate, w_up):
    g1 = lax.ppermute(w_gate, "col", y_perm(1))
    u2 = lax.ppermute(w_up, "col", y_perm(-1))
    u1 = lax.ppermute(w_up, "col", y_perm(1))
    g2 = lax.ppermute(w_gate, "col", y_perm(-1))
    g3 = lax.ppermute(g1, "col", y_perm(1))
    u3 = lax.ppermute(u2, "col", y_perm(-1))
    return [w_gate, g1, g2, g3], [w_up, u1, u2, u3]


def rows_of_ring(chunk):
    got, up, down = [chunk], chunk, chunk
    for _ in range(3):
        up = lax.ppermute(up, "row", z_perm(1))
        down = lax.ppermute(down, "row", z_perm(-1))
        got += [up, down]
    cut = 88
    first = lax.ppermute(up[:cut], "row", z_perm(1))
    second = lax.ppermute(down[cut:], "row", z_perm(-1))
    return got + [jnp.concatenate([first, second])]


RING = (0, -1, 1, -2, 2, -3, 3, 4)


def deal(expert_ids):
    tok_count = expert_ids.shape[0]
    lanes = 128
    blocks = tok_count // lanes
    ids = expert_ids.T.reshape(2, blocks, lanes)
    m0 = jnp.any(ids == 0, axis=0)
    m1 = jnp.any(ids == 1, axis=0)
    classes = jnp.stack([m0 & ~m1, m0 & m1, m1 & ~m0]).astype(jnp.bfloat16)
    lane = jnp.arange(lanes)
    before = (lane[:, None] < lane[None, :]).astype(jnp.bfloat16)
    inside = jnp.einsum("kbi,ij->kbj", classes, before, preferred_element_type=jnp.float32)
    sums = jnp.sum(classes.astype(jnp.float32), axis=2).astype(jnp.bfloat16)
    block = jnp.arange(blocks)
    earlier = (block[:, None] < block[None, :]).astype(jnp.bfloat16)
    start = jnp.einsum("kb,bc->kc", sums, earlier, preferred_element_type=jnp.float32)
    rank = (inside + start[:, :, None]).astype(jnp.int32)
    own = jnp.where(m1, jnp.where(m0, rank[1], rank[2]), rank[0]) & (SETS - 1)
    own = jnp.where(m0 | m1, own, -1)
    per = blocks // ROWS
    first = start.astype(jnp.int32).reshape(3, ROWS, per)[:, :, :1]
    first = jnp.broadcast_to(first, (3, ROWS, per)).reshape(3, blocks, 1)
    place = jnp.sum(below(rank, own[None]) - below(first, own[None]), axis=0)
    shape = (ROWS, tok_count // ROWS)
    return (
        rank.reshape(3, *shape),
        own.reshape(shape),
        place.reshape(shape),
        m0.reshape(shape),
        m1.reshape(shape),
    )


def shards(tokens, expert_ids, w_gate, w_up):
    row = lax.axis_index("row")
    col = lax.axis_index("col")
    layer = lax.axis_index("layer")
    y = col % SETS
    gates, ups = weights_of_ring(w_gate, w_up)

    rank, own, place, m0, m1 = deal(expert_ids)
    slot = (rank[0] + rank[1], rank[1] + rank[2])
    member = (m0, m1)

    mine = own == y
    at = jnp.where(mine, place, -1)
    at_here = lax.dynamic_index_in_dim(at, row, 0, keepdims=False)
    send = (jnp.arange(SEND)[:, None] == at_here[None, :]).astype(jnp.bfloat16)
    chunk = jnp.dot(send, tokens, preferred_element_type=jnp.float32).astype(jnp.bfloat16)
    chunks = rows_of_ring(chunk)

    blocks = jnp.arange(HALVES * SETS * QUARTERS)
    lists = []
    for e in range(2):
        in_set = mine & member[e]
        b = slot[e] // SLOTS_DEV
        seen = below(rank[e], y) + below(rank[e + 1], y)
        hit = in_set[None] & (slot[e][None] < blocks[:, None, None] * SLOTS_DEV)
        start = jnp.sum(hit.astype(jnp.int32), axis=(1, 2))
        base = jnp.sum(jnp.where(b[None] == blocks[:, None, None], start[:, None, None], 0), axis=0)
        part = (b % QUARTERS) ^ layer
        group = (part >> 1) + 2 * (part & 1)
        target = group * GROUP + (b // QUARTERS) * DEAL + seen - base
        lists.append(jnp.where(in_set, target + 1, 0))
    packed = jnp.stack(
        [lists[0] >> 5, lists[0] & 31, lists[1] >> 5, lists[1] & 31], axis=1
    ).astype(jnp.bfloat16)
    spread = (jnp.arange(SEND)[None, :, None] == at[:, None, :]).astype(jnp.bfloat16)
    moved = jnp.einsum("qvt,qpt->vqp", packed, spread, preferred_element_type=jnp.float32)
    moved = moved.astype(jnp.int32)
    ring = (row + jnp.array(RING)) % ROWS
    rows = jnp.arange(QUARTERS * GROUP)
    picks = []
    for e in range(2):
        target = jnp.take(moved[2 * e] * 32 + moved[2 * e + 1], ring, axis=0)
        picks.append((rows[:, None] + 1 == target.reshape(1, -1)).astype(jnp.bfloat16))

    b_own = col * QUARTERS + layer
    places = []
    for e in range(2):
        low = b_own * SLOTS_DEV
        in_block = member[e] & (slot[e] >= low) & (slot[e] < low + SLOTS_DEV)
        early = member[e] & (slot[e] < low)
        first = [
            jnp.sum((early & (m0 == (k < 2)) & (m1 == (k > 0))).astype(jnp.int32))
            for k in (e, e + 1)
        ]
        nth = sum(below(rank[e + i], own) - below(first[i], own) for i in range(2))
        slot_at = jnp.where(in_block, slot[e] - low, -1).reshape(1, -1)
        from_at = jnp.where(in_block, own * DEAL + nth, -1).reshape(1, -1)
        to = (jnp.arange(SLOTS_DEV)[:, None] == slot_at).astype(jnp.bfloat16)
        source = (jnp.arange(SETS * DEAL)[:, None] == from_at).astype(jnp.bfloat16)
        places.append(
            jnp.einsum("it,jt->ij", to, source, preferred_element_type=jnp.float32).astype(
                jnp.bfloat16
            )
        )

    early_chunks = jnp.concatenate(chunks[:-1])
    n_early = early_chunks.shape[0]
    results = []
    for e in range(2):
        x = jnp.dot(
            picks[e][:, :n_early], early_chunks, preferred_element_type=jnp.float32
        ) + jnp.dot(picks[e][:, n_early:], chunks[-1], preferred_element_type=jnp.float32)
        x = x.astype(jnp.bfloat16)
        w = jnp.concatenate([g[e] for g in gates] + [u[e] for u in ups], axis=1)
        sums = jnp.dot(x, w, preferred_element_type=jnp.float32)
        keep, give = sums[: 2 * GROUP], sums[2 * GROUP :]
        keep = keep + lax.ppermute(give, "layer", layer_perm(1))
        keep, give = keep[:GROUP], keep[GROUP:]
        keep = keep + lax.ppermute(give, "layer", layer_perm(2))
        half = keep.shape[1] // 2
        hidden = jax.nn.silu(keep[:, :half]) * keep[:, half:]
        results.append(hidden.astype(jnp.bfloat16))

    hidden = jnp.stack(results).reshape(2, GROUP, SETS, -1)
    order = jnp.array([(0, 2, 3, 1)])[0]
    pieces = [hidden[:, :, order[(a - y) % SETS]] for a in range(SETS)]
    hidden = jnp.concatenate(pieces, axis=-1)
    width = hidden.shape[-1]
    hidden = hidden.reshape(2, HALVES * SETS, DEAL, width).transpose(1, 0, 2, 3)
    hidden = lax.all_to_all(hidden, "col", 0, 0)
    hidden = hidden.reshape(HALVES, SETS, 2, DEAL, width)
    outs = []
    for e in range(2):
        for h in range(HALVES):
            rows_of = hidden[h, :, e].reshape(SETS * DEAL, width)
            outs.append(jnp.dot(places[e], rows_of, preferred_element_type=jnp.float32))
    return jnp.stack(
        [jnp.concatenate(outs[:2], axis=1), jnp.concatenate(outs[2:], axis=1)]
    ).astype(jnp.bfloat16)


def solution(mesh):
    in_specs = (
        P("row", "layer"),
        P(),
        P(None, "layer", ("row", "col")),
        P(None, "layer", ("row", "col")),
    )
    out_specs = P(None, ("col", "layer"), "row")
    return jax.shard_map(shards, mesh=mesh, in_specs=in_specs, out_specs=out_specs, check_vma=False)
```

```python
import jax
import jax.numpy as jnp
from jax import lax
from jax.experimental import pallas as pl
from jax.experimental.pallas import tpu as pltpu
from jax.sharding import PartitionSpec as P


ROWS = 8
SETS = 4
HALVES = 2
QUARTERS = 4
SLOTS_DEV = 80
SEND = 168
DEAL = 21
GROUP = HALVES * SETS * DEAL
DEAL_PAD = 24
STEPS = 256
TOP = 32767.0


def y_perm(step):
    return [(y, (y + step) % SETS) for y in range(SETS)]


def y_cross_perm(step):
    return [(2 * y + k, 2 * ((y + step) % SETS) + 1 - k) for y in range(SETS) for k in range(2)]


def z_perm(step):
    return [(z, (z + step) % ROWS) for z in range(ROWS)]


SWAP = [(0, 1), (1, 0)]


def below(n, s):
    return (n + (SETS - 1) - s) >> 2


def pick_of(pair, index):
    return lax.dynamic_index_in_dim(pair, index, 0, keepdims=False)


def weights_of_ring(w_gate, w_up, core):
    near = jnp.stack([pick_of(w_gate, core), pick_of(w_up, core)])
    far = jnp.stack([pick_of(w_gate, 1 - core), pick_of(w_up, 1 - core)])
    near1 = lax.ppermute(near, "y", y_perm(1))
    far2 = lax.ppermute(far, ("y", "core"), y_cross_perm(-1))
    far1 = lax.ppermute(far, ("y", "core"), y_cross_perm(1))
    near2 = lax.ppermute(near, "y", y_perm(-1))
    far0 = lax.ppermute(far, "core", SWAP)
    near3 = lax.ppermute(near1, "y", y_perm(1))
    far3 = lax.ppermute(far2, "y", y_perm(-1))
    return [near, near1, near2, near3], [far0, far1, far2, far3]


def rows_of_ring(chunk):
    got, up, down = [chunk], chunk, chunk
    for _ in range(1, 4):
        up = lax.ppermute(up, "z", z_perm(1))
        down = lax.ppermute(down, "z", z_perm(-1))
        got += [up, down]
    cut = 88
    first = lax.ppermute(up[:cut], "z", z_perm(1))
    second = lax.ppermute(down[cut:], "z", z_perm(-1))
    return got + [jnp.concatenate([first, second])]


LANES = 128
VMEM = pl.BlockSpec(memory_space=pltpu.VMEM)
SMEM = pl.BlockSpec(memory_space=pltpu.SMEM)


def iota(shape, dim):
    return lax.broadcasted_iota(jnp.int32, shape, dim)


def exact_dot(a, b):
    return jnp.dot(a.astype(jnp.bfloat16), b.astype(jnp.bfloat16), preferred_element_type=jnp.float32)


def rows_product(a, b):
    return lax.dot_general(a, b, (((1,), (1,)), ((), ())), preferred_element_type=jnp.float32)


def one_hot(values, count):
    wide = [
        (iota((count, LANES), 0) == values[i : i + 1]).astype(jnp.float32).astype(jnp.bfloat16)
        for i in range(values.shape[0])
    ]
    return jnp.concatenate(wide, axis=1)


def deal_kernel(here, code, tokens, chunk, rank, own, at):
    blocks = code.shape[0]
    per = blocks // ROWS
    kinds = [(code[...] == k).astype(jnp.float32) for k in (1, 3, 2)]
    before = (iota((LANES, LANES), 0) < iota((LANES, LANES), 1)).astype(jnp.float32)
    ones = jnp.ones((LANES, LANES), jnp.float32)
    r, c = iota((blocks, blocks), 0), iota((blocks, blocks), 1)
    earlier = (c < r).astype(jnp.float32)
    planes = (c < r // per * per).astype(jnp.float32)
    ranks, firsts = [], []
    for kind in kinds:
        sums = exact_dot(kind, ones)
        ranks.append((exact_dot(kind, before) + exact_dot(earlier, sums)).astype(jnp.int32))
        firsts.append(exact_dot(planes, sums).astype(jnp.int32))
    which = jnp.where(code[...] == 3, ranks[1], jnp.where(code[...] == 2, ranks[2], ranks[0]))
    mod = jnp.where(code[...] > 0, which & (SETS - 1), -1)
    place = sum(below(n, mod) - below(f, mod) for n, f in zip(ranks, firsts))
    place = jnp.where(mod == here[1], place, -1)
    own[...] = mod
    for k in range(3):
        rank[k] = ranks[k]
    for q in range(ROWS):
        at[q, :per] = place[q * per : (q + 1) * per]
    send = one_hot(at[here[0]][:per], SEND)
    chunk[...] = jnp.dot(send, tokens[...], preferred_element_type=jnp.float32).astype(jnp.bfloat16)


def lists_kernel(here, code, rank, own, at, lists, places):
    z, y, low, group_here, core = (here[i] for i in range(5))
    per = code.shape[0] // ROWS
    n_blocks = HALVES * SETS * QUARTERS
    mine = own[...] == y
    targets, slot_at, from_at = [], [], []
    for e in range(2):
        member = (code[...] == 1 + e) | (code[...] == 3)
        slot = rank[e] + rank[e + 1]
        seen = below(rank[e], y) + below(rank[e + 1], y)
        in_set = mine & member
        base = jnp.zeros_like(slot)
        for b in range(1, n_blocks):
            count = jnp.sum((in_set & (slot < b * SLOTS_DEV)).astype(jnp.int32))
            base = jnp.where(slot >= b * SLOTS_DEV, count, base)
        b = (slot * 52429) >> 22
        group = (b & (QUARTERS - 1)) ^ group_here
        target = group * GROUP + (b >> 2) * DEAL + seen - base
        targets.append(jnp.where(in_set, target + 1, 0))
        inside = member & (slot >= low) & (slot < low + SLOTS_DEV)
        early = member & (slot < low)
        nth = own[...] * DEAL_PAD
        for k, kind in ((e, 1 if e == 0 else 3), (e + 1, 3 if e == 0 else 2)):
            first = jnp.sum((early & (code[...] == kind)).astype(jnp.int32))
            nth += below(rank[k], own[...]) - below(first, own[...])
        slot_at.append(jnp.where(inside, slot - low, -1))
        from_at.append(jnp.where(inside, nth, -1))
    own_expert = jnp.where(core == 0, targets[0], targets[1])
    other = jnp.where(core == 0, targets[1], targets[0])
    turned = jnp.where((other - 1) // GROUP % 2 == 0, other + GROUP, other - GROUP)
    other = jnp.where(other > 0, turned, 0)
    parts = [own_expert >> 5, own_expert & 31, other >> 5, other & 31]
    parts = [p.astype(jnp.float32).astype(jnp.bfloat16) for p in parts]
    for q in range(ROWS):
        distance = (q - z + ROWS) & (ROWS - 1)
        turn = jnp.where(distance <= ROWS // 2, 2 * distance, 2 * (ROWS - distance) - 1)
        turn = jnp.where(distance == ROWS // 2, ROWS - 1, turn)
        span = slice(q * per, (q + 1) * per)
        values = [jnp.concatenate([p[i : i + 1] for i in range(q * per, (q + 1) * per)], axis=1) for p in parts]
        values = jnp.concatenate(values + values, axis=0)
        spread = one_hot(at[q][:per], SEND)
        lists[turn] = rows_product(values, spread)
    for i in range(2):
        total = jnp.zeros(places.shape[1:], jnp.float32)
        for q in range(ROWS):
            span = slice(q * per, (q + 1) * per)
            total += rows_product(
                one_hot(slot_at[i][span], SLOTS_DEV), one_hot(from_at[i][span], SETS * DEAL_PAD)
            )
        places[i] = total.astype(jnp.bfloat16)


def coded(values, out, column):
    rows = values.shape[0]
    top = jnp.maximum(jnp.max(jnp.abs(values), axis=1, keepdims=True), 1e-37)
    log = jnp.ceil(jnp.log2(top) * STEPS)
    parts = jnp.clip(values * (TOP * jnp.exp2(log * (-1.0 / STEPS))), -TOP, TOP)
    span = slice(column * LANES, (column + 1) * LANES)
    out[:rows, span] = jnp.round(parts).astype(jnp.int32).astype(jnp.int16)
    tail = jnp.zeros((out.shape[0] - rows, LANES), jnp.float32)
    for i in range(0, rows, LANES):
        some = log[i : i + LANES]
        there = iota((some.shape[0], LANES), 0) == iota((some.shape[0], LANES), 1)
        line = jnp.sum(jnp.where(there, some, 0.0), axis=0, keepdims=True)
        tail = jnp.where(iota(tail.shape, 0) == i // LANES, line, tail)
    out[rows:, span] = tail.astype(jnp.int32).astype(jnp.int16)


def decoded(code, column, rows):
    span = slice(column * LANES, (column + 1) * LANES)
    tail = code[rows:, span].astype(jnp.int32).astype(jnp.float32)
    logs = []
    for i in range(0, rows, LANES):
        count = min(LANES, rows - i)
        there = iota((count, LANES), 0) == iota((count, LANES), 1)
        line = tail[i // LANES : i // LANES + 1]
        logs.append(jnp.sum(jnp.where(there, line, 0.0), axis=1, keepdims=True))
    scale = jnp.exp2(jnp.concatenate(logs, axis=0) * (1.0 / STEPS)) * (1.0 / TOP)
    return code[:rows, span].astype(jnp.int32).astype(jnp.float32) * scale


def product_kernel(x, *refs):
    count = (len(refs) - 2) // 2
    near, far, keep, give = refs[:count], refs[count : 2 * count], refs[-2], refs[-1]
    n_half = keep.shape[0]
    for j, (a, b) in enumerate(zip(near, far)):
        w = jnp.concatenate(
            [jnp.concatenate([a[0], a[1]], axis=1), jnp.concatenate([b[0], b[1]], axis=1)], axis=0
        )
        sums = jnp.dot(x[n_half:], w, preferred_element_type=jnp.float32)
        for i in range(2):
            coded(sums[:, i * LANES : (i + 1) * LANES], give, 2 * j + i)
        sums = jnp.dot(x[:n_half], w, preferred_element_type=jnp.float32)
        keep[:, 2 * j * LANES : 2 * (j + 1) * LANES] = sums


def product(x, near, far):
    rows, depth = x.shape
    width = len(near) * 2 * near[0].shape[2]
    return pl.pallas_call(
        product_kernel,
        out_shape=(
            jax.ShapeDtypeStruct((rows // 2, width), jnp.float32),
            jax.ShapeDtypeStruct((rows // 2 + 16, width), jnp.int16),
        ),
        in_specs=[VMEM] * (1 + 2 * len(near)),
        out_specs=(VMEM,) * 2,
        compiler_params=pltpu.CompilerParams(vmem_limit_bytes=24 << 20),
        cost_estimate=pl.CostEstimate(
            flops=2 * rows * depth * width,
            bytes_accessed=4 * rows * width + 2 * depth * (rows + width),
            transcendentals=0,
        ),
    )(x, *near, *far)


def gated_kernel(here, *refs):
    keeps, codes, out = refs[:2], refs[2:4], refs[4]
    rows = keeps[0].shape[0]
    y, core = here[1], here[4]
    for o, ahead in enumerate((0, SETS - 1, 1, 2)):
        keep, code, j = keeps[o // 2], codes[o // 2], o % 2
        gate, up = (
            keep[:, (2 * j + i) * LANES : (2 * j + i + 1) * LANES] + decoded(code, 2 * j + i, rows)
            for i in range(2)
        )
        hidden = gate / (1.0 + jnp.exp(-gate)) * up
        piece = (y + ahead) & (SETS - 1)
        pad = jnp.zeros((DEAL_PAD - DEAL, LANES), jnp.float32)
        for k in range(2):
            for c in range(HALVES * SETS):
                first = k * GROUP + c * DEAL
                some = jnp.concatenate([hidden[first : first + DEAL], pad], axis=0)
                out[2 * c + (k ^ core), piece] = some.astype(jnp.bfloat16)


def placed_kernel(got, places, out):
    for e in range(2):
        for h in range(HALVES):
            lines = [
                jnp.concatenate([got[(h * SETS + s) * 2 + e, p] for p in range(SETS)], axis=1)
                for s in range(SETS)
            ]
            rows = jnp.concatenate(lines, axis=0)
            wide = rows.shape[1]
            out[e, :, h * wide : (h + 1) * wide] = jnp.dot(
                places[e], rows, preferred_element_type=jnp.float32
            ).astype(jnp.bfloat16)


def shards(tokens, expert_ids, w_gate, w_up):
    z = lax.axis_index("z")
    y = lax.axis_index("y")
    x_lo = lax.axis_index("x_lo")
    x_hi = lax.axis_index("x_hi")
    core = lax.axis_index("core")
    near, far = weights_of_ring(w_gate, w_up, core)

    blocks = expert_ids.shape[0] // LANES
    ids = expert_ids.T
    code = sum(jnp.any(ids == e, axis=0).astype(jnp.int32) * (1 + e) for e in range(2))
    code = code.reshape(blocks, LANES)
    low = ((x_lo * SETS + y) * QUARTERS + 2 * x_hi + core) * SLOTS_DEV
    here = jnp.stack([z, y, low, 2 * x_hi + core, core]).astype(jnp.int32)
    chunk, rank, own, at = pl.pallas_call(
        deal_kernel,
        out_shape=(
            jax.ShapeDtypeStruct((SEND, tokens.shape[1]), jnp.bfloat16),
            jax.ShapeDtypeStruct((3, blocks, LANES), jnp.int32),
            jax.ShapeDtypeStruct((blocks, LANES), jnp.int32),
            jax.ShapeDtypeStruct((ROWS, 8, LANES), jnp.int32),
        ),
        in_specs=[SMEM, VMEM, VMEM],
        out_specs=(VMEM,) * 4,
        compiler_params=pltpu.CompilerParams(vmem_limit_bytes=8 << 20),
        cost_estimate=pl.CostEstimate(flops=1 << 30, bytes_accessed=1 << 22, transcendentals=0),
    )(here, code, tokens)
    chunks = rows_of_ring(chunk)

    moved, places = pl.pallas_call(
        lists_kernel,
        out_shape=(
            jax.ShapeDtypeStruct((ROWS, 8, SEND), jnp.float32),
            jax.ShapeDtypeStruct((2, SLOTS_DEV, SETS * DEAL_PAD), jnp.bfloat16),
        ),
        in_specs=[SMEM] + [VMEM] * 4,
        out_specs=(VMEM,) * 2,
        compiler_params=pltpu.CompilerParams(vmem_limit_bytes=8 << 20),
        cost_estimate=pl.CostEstimate(flops=1 << 30, bytes_accessed=1 << 20, transcendentals=0),
    )(here, code, rank, own, at)
    moved = moved.astype(jnp.int32)
    rows = jnp.arange(QUARTERS * GROUP)
    pick, other = (
        (rows[:, None] + 1 == (moved[:, 2 * i] * 32 + moved[:, 2 * i + 1]).reshape(1, -1)).astype(
            jnp.bfloat16
        )
        for i in range(2)
    )

    both = jnp.concatenate([pick, other])
    n_rows = QUARTERS * GROUP
    soon = jnp.dot(
        both[:, : 5 * SEND], jnp.concatenate(chunks[:5]), preferred_element_type=jnp.float32
    ).astype(jnp.bfloat16)
    soon, *middle = lax.optimization_barrier((soon, *chunks[5:7]))
    soon = jnp.dot(
        both[:, 5 * SEND : 7 * SEND],
        jnp.concatenate(middle),
        preferred_element_type=jnp.float32,
    ).astype(jnp.bfloat16) + soon
    soon = lax.optimization_barrier(soon)
    early_b = lax.ppermute(soon[n_rows:], "core", SWAP)
    late_b = lax.ppermute(chunks[-1], "core", SWAP)
    late = pick[:, 7 * SEND :]
    x = jnp.concatenate(
        [
            early + jnp.dot(late, rest, preferred_element_type=jnp.float32).astype(jnp.bfloat16)
            for early, rest in ((soon[:n_rows], chunks[-1]), (early_b, late_b))
        ],
        axis=1,
    )

    keeps, gots = [], []
    for part in range(2):
        some = slice(2 * part, 2 * part + 2)
        keep, give = product(x, near[some], far[some])
        keeps.append(keep)
        gots.append(lax.ppermute(give, "x_hi", SWAP))
    hidden = pl.pallas_call(
        gated_kernel,
        out_shape=jax.ShapeDtypeStruct((2 * HALVES * SETS, SETS, DEAL_PAD, LANES), jnp.bfloat16),
        in_specs=[SMEM] + [VMEM] * 4,
        out_specs=VMEM,
        compiler_params=pltpu.CompilerParams(vmem_limit_bytes=16 << 20),
        cost_estimate=pl.CostEstimate(flops=1 << 30, bytes_accessed=1 << 22, transcendentals=0),
    )(here, *keeps, *gots)
    hidden = lax.all_to_all(hidden, ("x_lo", "y", "core"), 0, 0)
    return pl.pallas_call(
        placed_kernel,
        out_shape=jax.ShapeDtypeStruct((2, SLOTS_DEV, HALVES * SETS * LANES), jnp.bfloat16),
        in_specs=[VMEM] * 2,
        out_specs=VMEM,
        compiler_params=pltpu.CompilerParams(vmem_limit_bytes=8 << 20),
        cost_estimate=pl.CostEstimate(flops=1 << 28, bytes_accessed=1 << 20, transcendentals=0),
    )(hidden, places)


def solution(mesh):
    cut = jax.sharding.Mesh(
        mesh.devices.reshape(ROWS, HALVES, SETS, 2, 2), ("z", "x_lo", "y", "x_hi", "core")
    )
    layer, col = ("x_hi", "core"), ("x_lo", "y")
    in_specs = (P("z", layer), P(), P(None, layer, ("z", *col)), P(None, layer, ("z", *col)))
    out_specs = P(None, (*col, *layer), "z")
    return jax.shard_map(shards, mesh=cut, in_specs=in_specs, out_specs=out_specs, check_vma=False)
```

```python
import jax
import jax.numpy as jnp
from jax import lax
from jax.experimental import pallas as pl
from jax.experimental.pallas import tpu as pltpu
from jax.sharding import PartitionSpec as P


ROWS = 8
SETS = 4
HALVES = 2
QUARTERS = 4
SLOTS_DEV = 80
SEND = 168
DEAL = 21
GROUP = HALVES * SETS * DEAL
DEAL_PAD = 24
COPIES = 8
STEPS = 256
TOP = 32767.0


def y_perm(step):
    return [(y, (y + step) % SETS) for y in range(SETS)]


def y_cross_perm(step):
    return [(2 * y + k, 2 * ((y + step) % SETS) + 1 - k) for y in range(SETS) for k in range(2)]


def z_perm(step):
    return [(z, (z + step) % ROWS) for z in range(ROWS)]


SWAP = [(0, 1), (1, 0)]


def below(n, s):
    return (n + (SETS - 1) - s) >> 2


def pick_of(pair, index):
    return lax.dynamic_index_in_dim(pair, index, 0, keepdims=False)


def weights_of_ring(w_gate, w_up, core):
    near = jnp.stack([pick_of(w_gate, core), pick_of(w_up, core)])
    far = jnp.stack([pick_of(w_gate, 1 - core), pick_of(w_up, 1 - core)])
    near1 = lax.ppermute(near, "y", y_perm(1))
    far2 = lax.ppermute(far, ("y", "core"), y_cross_perm(-1))
    far1 = lax.ppermute(far, ("y", "core"), y_cross_perm(1))
    near2 = lax.ppermute(near, "y", y_perm(-1))
    far0 = lax.ppermute(far, "core", SWAP)
    near3 = lax.ppermute(near1, "y", y_perm(1))
    far3 = lax.ppermute(far2, "y", y_perm(-1))
    return [near, near1, near2, near3], [far0, far1, far2, far3]


def rows_of_ring(chunk):
    got, up, down = [chunk], chunk, chunk
    for _ in range(1, 4):
        up = lax.ppermute(up, "z", z_perm(1))
        down = lax.ppermute(down, "z", z_perm(-1))
        got += [up, down]
    cut = 88
    first = lax.ppermute(up[:cut], "z", z_perm(1))
    second = lax.ppermute(down[cut:], "z", z_perm(-1))
    return got + [jnp.concatenate([first, second])]


LANES = 128
VMEM = pl.BlockSpec(memory_space=pltpu.VMEM)
SMEM = pl.BlockSpec(memory_space=pltpu.SMEM)


def iota(shape, dim):
    return lax.broadcasted_iota(jnp.int32, shape, dim)


def exact_dot(a, b):
    return jnp.dot(a.astype(jnp.bfloat16), b.astype(jnp.bfloat16), preferred_element_type=jnp.float32)


def rows_product(a, b):
    return lax.dot_general(a, b, (((1,), (1,)), ((), ())), preferred_element_type=jnp.float32)


def one_hot(values, count):
    wide = [
        (iota((count, LANES), 0) == values[i : i + 1]).astype(jnp.float32).astype(jnp.bfloat16)
        for i in range(values.shape[0])
    ]
    return jnp.concatenate(wide, axis=1)


def deal_kernel(ids, tokens, chunk, code, rank, own, at, held, arrived):
    blocks = code.shape[0]
    per = blocks // ROWS
    share = tokens.shape[0] // COPIES
    copies = [
        pltpu.make_async_copy(
            tokens.at[pl.ds(i * share, share)], held.at[pl.ds(i * share, share)], arrived.at[i]
        )
        for i in range(COPIES)
    ]
    for copy in copies:
        copy.start()
    named = [((ids[0:1] == e) | (ids[1:2] == e)).astype(jnp.int32) * (1 + e) for e in range(2)]
    named = named[0] + named[1]
    code[...] = jnp.concatenate(
        [named[:, i * LANES : (i + 1) * LANES] for i in range(blocks)], axis=0
    )
    kinds = [(code[...] == k).astype(jnp.float32) for k in (1, 3, 2)]
    before = (iota((LANES, LANES), 0) < iota((LANES, LANES), 1)).astype(jnp.float32)
    ones = jnp.ones((LANES, LANES), jnp.float32)
    r, c = iota((blocks, blocks), 0), iota((blocks, blocks), 1)
    earlier = (c < r).astype(jnp.float32)
    planes = (c < r // per * per).astype(jnp.float32)
    ranks, firsts = [], []
    for kind in kinds:
        sums = exact_dot(kind, ones)
        ranks.append((exact_dot(kind, before) + exact_dot(earlier, sums)).astype(jnp.int32))
        firsts.append(exact_dot(planes, sums).astype(jnp.int32))
    which = jnp.where(code[...] == 3, ranks[1], jnp.where(code[...] == 2, ranks[2], ranks[0]))
    mod = jnp.where(code[...] > 0, which & (SETS - 1), -1)
    place = sum(below(n, mod) - below(f, mod) for n, f in zip(ranks, firsts))
    place = jnp.where(mod == lax.axis_index("y"), place, -1)
    own[...] = mod
    for k in range(3):
        rank[k] = ranks[k]
    for q in range(ROWS):
        at[q, :per] = place[q * per : (q + 1) * per]
    send = one_hot(at[lax.axis_index("z")][:per], SEND)
    for copy in copies:
        copy.wait()
    chunk[...] = jnp.dot(send, held[...], preferred_element_type=jnp.float32).astype(jnp.bfloat16)


def lists_kernel(here, code, rank, own, at, lists, places):
    z, y, low, group_here, core = (here[i] for i in range(5))
    per = code.shape[0] // ROWS
    n_blocks = HALVES * SETS * QUARTERS
    mine = own[...] == y
    targets, slot_at, from_at = [], [], []
    for e in range(2):
        member = (code[...] == 1 + e) | (code[...] == 3)
        slot = rank[e] + rank[e + 1]
        seen = below(rank[e], y) + below(rank[e + 1], y)
        in_set = mine & member
        base = jnp.zeros_like(slot)
        for b in range(1, n_blocks):
            count = jnp.sum((in_set & (slot < b * SLOTS_DEV)).astype(jnp.int32))
            base = jnp.where(slot >= b * SLOTS_DEV, count, base)
        b = (slot * 52429) >> 22
        group = (b & (QUARTERS - 1)) ^ group_here
        target = group * GROUP + (b >> 2) * DEAL + seen - base
        targets.append(jnp.where(in_set, target + 1, 0))
        inside = member & (slot >= low) & (slot < low + SLOTS_DEV)
        early = member & (slot < low)
        nth = own[...] * DEAL_PAD
        for k, kind in ((e, 1 if e == 0 else 3), (e + 1, 3 if e == 0 else 2)):
            first = jnp.sum((early & (code[...] == kind)).astype(jnp.int32))
            nth += below(rank[k], own[...]) - below(first, own[...])
        slot_at.append(jnp.where(inside, slot - low, -1))
        from_at.append(jnp.where(inside, nth, -1))
    own_expert = jnp.where(core == 0, targets[0], targets[1])
    other = jnp.where(core == 0, targets[1], targets[0])
    turned = jnp.where((other - 1) // GROUP % 2 == 0, other + GROUP, other - GROUP)
    other = jnp.where(other > 0, turned, 0)
    parts = [own_expert >> 5, own_expert & 31, other >> 5, other & 31]
    parts = [p.astype(jnp.float32).astype(jnp.bfloat16) for p in parts]
    for q in range(ROWS):
        distance = (q - z + ROWS) & (ROWS - 1)
        turn = jnp.where(distance <= ROWS // 2, 2 * distance, 2 * (ROWS - distance) - 1)
        turn = jnp.where(distance == ROWS // 2, ROWS - 1, turn)
        span = slice(q * per, (q + 1) * per)
        values = [jnp.concatenate([p[i : i + 1] for i in range(q * per, (q + 1) * per)], axis=1) for p in parts]
        values = jnp.concatenate(values + values, axis=0)
        spread = one_hot(at[q][:per], SEND)
        lists[turn] = rows_product(values, spread)
    for i in range(2):
        total = jnp.zeros(places.shape[1:], jnp.float32)
        for q in range(ROWS):
            span = slice(q * per, (q + 1) * per)
            total += rows_product(
                one_hot(slot_at[i][span], SLOTS_DEV), one_hot(from_at[i][span], SETS * DEAL_PAD)
            )
        places[i] = total.astype(jnp.bfloat16)


def coded(values, out, column):
    rows = values.shape[0]
    top = jnp.maximum(jnp.max(jnp.abs(values), axis=1, keepdims=True), 1e-37)
    log = jnp.ceil(jnp.log2(top) * STEPS)
    parts = jnp.clip(values * (TOP * jnp.exp2(log * (-1.0 / STEPS))), -TOP, TOP)
    span = slice(column * LANES, (column + 1) * LANES)
    out[:rows, span] = jnp.round(parts).astype(jnp.int32).astype(jnp.int16)
    tail = jnp.zeros((out.shape[0] - rows, LANES), jnp.float32)
    for i in range(0, rows, LANES):
        some = log[i : i + LANES]
        there = iota((some.shape[0], LANES), 0) == iota((some.shape[0], LANES), 1)
        line = jnp.sum(jnp.where(there, some, 0.0), axis=0, keepdims=True)
        tail = jnp.where(iota(tail.shape, 0) == i // LANES, line, tail)
    out[rows:, span] = tail.astype(jnp.int32).astype(jnp.int16)


def decoded(code, column, rows):
    span = slice(column * LANES, (column + 1) * LANES)
    tail = code[rows:, span].astype(jnp.int32).astype(jnp.float32)
    logs = []
    for i in range(0, rows, LANES):
        count = min(LANES, rows - i)
        there = iota((count, LANES), 0) == iota((count, LANES), 1)
        line = tail[i // LANES : i // LANES + 1]
        logs.append(jnp.sum(jnp.where(there, line, 0.0), axis=1, keepdims=True))
    scale = jnp.exp2(jnp.concatenate(logs, axis=0) * (1.0 / STEPS)) * (1.0 / TOP)
    return code[:rows, span].astype(jnp.int32).astype(jnp.float32) * scale


def piece_sums(xs, span, near, far):
    x = jnp.concatenate([x[span] for x in xs], axis=1)
    w = jnp.concatenate([jnp.concatenate([w[0], w[1]], axis=1) for w in (near, far)], axis=0)
    return jnp.dot(x, w, preferred_element_type=jnp.float32)


def give_kernel(xa, xb, *refs):
    count = (len(refs) - 2) // 2
    for j in range(count):
        sums = piece_sums((xa, xb), slice(2 * GROUP, 4 * GROUP), refs[j], refs[count + j])
        for k in range(2):
            for i in range(2):
                some = sums[k * GROUP : (k + 1) * GROUP, i * LANES : (i + 1) * LANES]
                coded(some, refs[2 * count + k], 2 * j + i)


def keep_kernel(xa, xb, *refs):
    count = (len(refs) - 2) // 2
    for j in range(count):
        sums = piece_sums((xa, xb), slice(0, 2 * GROUP), refs[j], refs[count + j])
        for k in range(2):
            refs[2 * count + k][:, 2 * j * LANES : 2 * (j + 1) * LANES] = sums[
                k * GROUP : (k + 1) * GROUP
            ]


def product(kernel, xs, near, far, rows, kind):
    depth = 2 * xs[0].shape[1]
    width = len(near) * 2 * LANES
    return pl.pallas_call(
        kernel,
        out_shape=(jax.ShapeDtypeStruct((rows, width), kind),) * 2,
        in_specs=[VMEM] * (2 + 2 * len(near)),
        out_specs=(VMEM,) * 2,
        compiler_params=pltpu.CompilerParams(vmem_limit_bytes=24 << 20),
        cost_estimate=pl.CostEstimate(
            flops=4 * GROUP * depth * width,
            bytes_accessed=8 * GROUP * width + 2 * depth * (2 * GROUP + width),
            transcendentals=0,
        ),
    )(*xs, *near, *far)


def gated_kernel(here, *refs):
    keeps, codes, out = refs[:2], refs[2:6], refs[6]
    rows = keeps[0].shape[0]
    y, core = here[1], here[4]
    for o, ahead in enumerate((0, SETS - 1, 1, 2)):
        piece = (y + ahead) & (SETS - 1)
        pad = jnp.zeros((DEAL_PAD - DEAL, LANES), jnp.float32)
        for k in range(2):
            gate, up = (
                keeps[k][:, (2 * o + i) * LANES : (2 * o + i + 1) * LANES]
                + decoded(codes[2 * (o // 2) + k], 2 * (o % 2) + i, rows)
                for i in range(2)
            )
            hidden = gate / (1.0 + jnp.exp(-gate)) * up
            for c in range(HALVES * SETS):
                some = jnp.concatenate([hidden[c * DEAL : (c + 1) * DEAL], pad], axis=0)
                out[c, k ^ core, piece] = some.astype(jnp.bfloat16)


def placed_kernel(got, places, out):
    for e in range(2):
        for h in range(HALVES):
            lines = [
                jnp.concatenate([got[h * SETS + s, e, p] for p in range(SETS)], axis=1)
                for s in range(SETS)
            ]
            rows = jnp.concatenate(lines, axis=0)
            wide = rows.shape[1]
            out[e, :, h * wide : (h + 1) * wide] = jnp.dot(
                places[e], rows, preferred_element_type=jnp.float32
            ).astype(jnp.bfloat16)


def shards(tokens, expert_ids, w_gate, w_up):
    z = lax.axis_index("z")
    y = lax.axis_index("y")
    x_lo = lax.axis_index("x_lo")
    x_hi = lax.axis_index("x_hi")
    core = lax.axis_index("core")
    near, far = weights_of_ring(w_gate, w_up, core)

    blocks = expert_ids.shape[0] // LANES
    low = ((x_lo * SETS + y) * QUARTERS + 2 * x_hi + core) * SLOTS_DEV
    here = jnp.stack([z, y, low, 2 * x_hi + core, core]).astype(jnp.int32)
    chunk, code, rank, own, at = pl.pallas_call(
        deal_kernel,
        out_shape=(
            jax.ShapeDtypeStruct((SEND, tokens.shape[1]), jnp.bfloat16),
            jax.ShapeDtypeStruct((blocks, LANES), jnp.int32),
            jax.ShapeDtypeStruct((3, blocks, LANES), jnp.int32),
            jax.ShapeDtypeStruct((blocks, LANES), jnp.int32),
            jax.ShapeDtypeStruct((ROWS, 8, LANES), jnp.int32),
        ),
        in_specs=[VMEM, pl.BlockSpec(memory_space=pl.ANY)],
        out_specs=(VMEM,) * 5,
        scratch_shapes=[
            pltpu.VMEM(tokens.shape, jnp.bfloat16),
            pltpu.SemaphoreType.DMA((COPIES,)),
        ],
        compiler_params=pltpu.CompilerParams(vmem_limit_bytes=60 << 20),
        cost_estimate=pl.CostEstimate(flops=1 << 30, bytes_accessed=1 << 22, transcendentals=0),
    )(expert_ids.T, tokens)
    chunks = rows_of_ring(chunk)

    moved, places = pl.pallas_call(
        lists_kernel,
        out_shape=(
            jax.ShapeDtypeStruct((ROWS, 8, SEND), jnp.float32),
            jax.ShapeDtypeStruct((2, SLOTS_DEV, SETS * DEAL_PAD), jnp.bfloat16),
        ),
        in_specs=[SMEM] + [VMEM] * 4,
        out_specs=(VMEM,) * 2,
        compiler_params=pltpu.CompilerParams(vmem_limit_bytes=8 << 20),
        cost_estimate=pl.CostEstimate(flops=1 << 30, bytes_accessed=1 << 20, transcendentals=0),
    )(here, code, rank, own, at)
    moved = moved.astype(jnp.int32)
    rows = jnp.arange(QUARTERS * GROUP)
    pick, other = (
        (rows[:, None] + 1 == (moved[:, 2 * i] * 32 + moved[:, 2 * i + 1]).reshape(1, -1)).astype(
            jnp.bfloat16
        )
        for i in range(2)
    )

    both = jnp.concatenate([pick, other])
    n_rows = QUARTERS * GROUP
    soon = jnp.dot(
        both[:, : 5 * SEND], jnp.concatenate(chunks[:5]), preferred_element_type=jnp.float32
    ).astype(jnp.bfloat16)
    soon, *middle = lax.optimization_barrier((soon, *chunks[5:7]))
    soon = jnp.dot(
        both[:, 5 * SEND : 7 * SEND],
        jnp.concatenate(middle),
        preferred_element_type=jnp.float32,
    ).astype(jnp.bfloat16) + soon
    soon = lax.optimization_barrier(soon)
    early_b = lax.ppermute(soon[n_rows:], "core", SWAP)
    late_b = lax.ppermute(chunks[-1], "core", SWAP)
    late = pick[:, 7 * SEND :]
    xs = [
        early + jnp.dot(late, rest, preferred_element_type=jnp.float32).astype(jnp.bfloat16)
        for early, rest in ((soon[:n_rows], chunks[-1]), (early_b, late_b))
    ]

    gots = []
    for part in range(2):
        some = slice(2 * part, 2 * part + 2)
        same, cross = product(give_kernel, xs, near[some], far[some], GROUP + 8, jnp.int16)
        gots.append(lax.ppermute(same, "x_hi", SWAP))
        gots.append(lax.ppermute(cross, ("x_hi", "core"), [(i, 3 - i) for i in range(4)]))
    same, cross = product(keep_kernel, xs, near, far, GROUP, jnp.float32)
    cross = lax.ppermute(cross, "core", SWAP)
    hidden = pl.pallas_call(
        gated_kernel,
        out_shape=jax.ShapeDtypeStruct((HALVES * SETS, 2, SETS, DEAL_PAD, LANES), jnp.bfloat16),
        in_specs=[SMEM] + [VMEM] * 6,
        out_specs=VMEM,
        compiler_params=pltpu.CompilerParams(vmem_limit_bytes=16 << 20),
        cost_estimate=pl.CostEstimate(flops=1 << 30, bytes_accessed=1 << 22, transcendentals=0),
    )(here, same, cross, *gots)
    hidden = lax.all_to_all(hidden, ("x_lo", "y"), 0, 0)
    return pl.pallas_call(
        placed_kernel,
        out_shape=jax.ShapeDtypeStruct((2, SLOTS_DEV, HALVES * SETS * LANES), jnp.bfloat16),
        in_specs=[VMEM] * 2,
        out_specs=VMEM,
        compiler_params=pltpu.CompilerParams(vmem_limit_bytes=8 << 20),
        cost_estimate=pl.CostEstimate(flops=1 << 28, bytes_accessed=1 << 20, transcendentals=0),
    )(hidden, places)


def solution(mesh):
    cut = jax.sharding.Mesh(
        mesh.devices.reshape(ROWS, HALVES, SETS, 2, 2), ("z", "x_lo", "y", "x_hi", "core")
    )
    layer, col = ("x_hi", "core"), ("x_lo", "y")
    in_specs = (P("z", layer), P(), P(None, layer, ("z", *col)), P(None, layer, ("z", *col)))
    out_specs = P(None, (*col, *layer), "z")
    return jax.shard_map(shards, mesh=cut, in_specs=in_specs, out_specs=out_specs, check_vma=False)
```

```python
import functools

import jax
import jax.numpy as jnp
from jax import lax
from jax.experimental import pallas as pl
from jax.experimental.pallas import tpu as pltpu
from jax.sharding import PartitionSpec as P


ROWS = 8
SETS = 4
HALVES = 2
QUARTERS = 4
SLOTS_DEV = 80
SEND = 168
DEAL = 21
GROUP = HALVES * SETS * DEAL
DEAL_PAD = 24
COPIES = 5
STEPS = 256
TOP = 32767.0


def y_perm(step):
    return [(y, (y + step) % SETS) for y in range(SETS)]


def y_cross_perm(step):
    return [(2 * y + k, 2 * ((y + step) % SETS) + 1 - k) for y in range(SETS) for k in range(2)]


def z_perm(step):
    return [(z, (z + step) % ROWS) for z in range(ROWS)]


SWAP = [(0, 1), (1, 0)]


def below(n, s):
    return (n + (SETS - 1) - s) >> 2


def pick_of(pair, index):
    return lax.dynamic_index_in_dim(pair, index, 0, keepdims=False)


def weights_of_ring(w_gate, w_up, core):
    near = jnp.stack([pick_of(w_gate, core), pick_of(w_up, core)])
    far = jnp.stack([pick_of(w_gate, 1 - core), pick_of(w_up, 1 - core)])
    near1 = lax.ppermute(near, "y", y_perm(1))
    far2 = lax.ppermute(far, ("y", "core"), y_cross_perm(-1))
    far1 = lax.ppermute(far, ("y", "core"), y_cross_perm(1))
    near2 = lax.ppermute(near, "y", y_perm(-1))
    far0 = lax.ppermute(far, "core", SWAP)
    near3 = lax.ppermute(near1, "y", y_perm(1))
    far3 = lax.ppermute(far2, "y", y_perm(-1))
    return [near, near1, near2, near3], [far0, far1, far2, far3]


def rows_of_ring(chunk):
    got, up, down = [chunk], chunk, chunk
    for _ in range(1, 4):
        up = lax.ppermute(up, "z", z_perm(1))
        down = lax.ppermute(down, "z", z_perm(-1))
        got += [up, down]
    cut = 88
    first = lax.ppermute(up[:cut], "z", z_perm(1))
    second = lax.ppermute(down[cut:], "z", z_perm(-1))
    return got, [first, second]


LANES = 128
VMEM = pl.BlockSpec(memory_space=pltpu.VMEM)
SMEM = pl.BlockSpec(memory_space=pltpu.SMEM)


def iota(shape, dim):
    return lax.broadcasted_iota(jnp.int32, shape, dim)


def exact_dot(a, b):
    return jnp.dot(a.astype(jnp.bfloat16), b.astype(jnp.bfloat16), preferred_element_type=jnp.float32)


def rows_product(a, b):
    return lax.dot_general(a, b, (((1,), (1,)), ((), ())), preferred_element_type=jnp.float32)


def one_hot(values, count):
    wide = [
        (iota((count, LANES), 0) == values[i : i + 1]).astype(jnp.float32).astype(jnp.bfloat16)
        for i in range(values.shape[0])
    ]
    return jnp.concatenate(wide, axis=1)


def deal_kernel(ids, tokens, chunk, code, rank, own, at, held, arrived):
    blocks = code.shape[0]
    per = blocks // ROWS
    share = tokens.shape[0] // COPIES
    copies = [
        pltpu.make_async_copy(
            tokens.at[pl.ds(i * share, share)], held.at[pl.ds(i * share, share)], arrived.at[i]
        )
        for i in range(COPIES)
    ]
    for copy in copies:
        copy.start()
    named = [((ids[0:1] == e) | (ids[1:2] == e)).astype(jnp.int32) * (1 + e) for e in range(2)]
    named = named[0] + named[1]
    code[...] = jnp.concatenate(
        [named[:, i * LANES : (i + 1) * LANES] for i in range(blocks)], axis=0
    )
    kinds = [(code[...] == k).astype(jnp.float32) for k in (1, 3, 2)]
    before = (iota((LANES, LANES), 0) < iota((LANES, LANES), 1)).astype(jnp.float32)
    ones = jnp.ones((LANES, LANES), jnp.float32)
    r, c = iota((blocks, blocks), 0), iota((blocks, blocks), 1)
    earlier = (c < r).astype(jnp.float32)
    planes = (c < r // per * per).astype(jnp.float32)
    ranks, firsts = [], []
    for kind in kinds:
        sums = exact_dot(kind, ones)
        ranks.append((exact_dot(kind, before) + exact_dot(earlier, sums)).astype(jnp.int32))
        firsts.append(exact_dot(planes, sums).astype(jnp.int32))
    which = jnp.where(code[...] == 3, ranks[1], jnp.where(code[...] == 2, ranks[2], ranks[0]))
    mod = jnp.where(code[...] > 0, which & (SETS - 1), -1)
    place = sum(below(n, mod) - below(f, mod) for n, f in zip(ranks, firsts))
    place = jnp.where(mod == lax.axis_index("y"), place, -1)
    own[...] = mod
    for k in range(3):
        rank[k] = ranks[k]
    for q in range(ROWS):
        at[q, :per] = place[q * per : (q + 1) * per]
    send = one_hot(at[lax.axis_index("z")][:per], SEND)
    total = jnp.zeros(chunk.shape, jnp.float32)
    for i, copy in enumerate(copies):
        copy.wait()
        span = slice(i * share, (i + 1) * share)
        total += jnp.dot(send[:, span], held[span], preferred_element_type=jnp.float32)
    chunk[...] = total.astype(jnp.bfloat16)


def lists_kernel(here, code, rank, own, at, lists, places):
    z, y, low, group_here, core = (here[i] for i in range(5))
    per = code.shape[0] // ROWS
    n_blocks = HALVES * SETS * QUARTERS
    mine = own[...] == y
    targets, slot_at, from_at = [], [], []
    for e in range(2):
        member = (code[...] == 1 + e) | (code[...] == 3)
        slot = rank[e] + rank[e + 1]
        seen = below(rank[e], y) + below(rank[e + 1], y)
        in_set = mine & member
        base = jnp.zeros_like(slot)
        for b in range(1, n_blocks):
            count = jnp.sum((in_set & (slot < b * SLOTS_DEV)).astype(jnp.int32))
            base = jnp.where(slot >= b * SLOTS_DEV, count, base)
        b = (slot * 52429) >> 22
        group = (b & (QUARTERS - 1)) ^ group_here
        target = group * GROUP + (b >> 2) * DEAL + seen - base
        targets.append(jnp.where(in_set, target + 1, 0))
        inside = member & (slot >= low) & (slot < low + SLOTS_DEV)
        early = member & (slot < low)
        nth = own[...] * DEAL_PAD
        for k, kind in ((e, 1 if e == 0 else 3), (e + 1, 3 if e == 0 else 2)):
            first = jnp.sum((early & (code[...] == kind)).astype(jnp.int32))
            nth += below(rank[k], own[...]) - below(first, own[...])
        slot_at.append(jnp.where(inside, slot - low, -1))
        from_at.append(jnp.where(inside, nth, -1))
    own_expert = jnp.where(core == 0, targets[0], targets[1])
    other = jnp.where(core == 0, targets[1], targets[0])
    turned = jnp.where((other - 1) // GROUP % 2 == 0, other + GROUP, other - GROUP)
    other = jnp.where(other > 0, turned, 0)
    parts = [own_expert >> 5, own_expert & 31, other >> 5, other & 31]
    parts = [p.astype(jnp.float32).astype(jnp.bfloat16) for p in parts]
    for q in range(ROWS):
        distance = (q - z + ROWS) & (ROWS - 1)
        turn = jnp.where(distance <= ROWS // 2, 2 * distance, 2 * (ROWS - distance) - 1)
        turn = jnp.where(distance == ROWS // 2, ROWS - 1, turn)
        span = slice(q * per, (q + 1) * per)
        values = [jnp.concatenate([p[i : i + 1] for i in range(q * per, (q + 1) * per)], axis=1) for p in parts]
        values = jnp.concatenate(values + values, axis=0)
        spread = one_hot(at[q][:per], SEND)
        lists[turn] = rows_product(values, spread)
    for i in range(2):
        total = jnp.zeros(places.shape[1:], jnp.float32)
        for q in range(ROWS):
            span = slice(q * per, (q + 1) * per)
            total += rows_product(
                one_hot(slot_at[i][span], SLOTS_DEV), one_hot(from_at[i][span], SETS * DEAL_PAD)
            )
        places[i] = total.astype(jnp.bfloat16)


def coded(values, out, column):
    rows = values.shape[0]
    top = jnp.maximum(jnp.max(jnp.abs(values), axis=1, keepdims=True), 1e-37)
    log = jnp.ceil(jnp.log2(top) * STEPS)
    parts = jnp.clip(values * (TOP * jnp.exp2(log * (-1.0 / STEPS))), -TOP, TOP)
    span = slice(column * LANES, (column + 1) * LANES)
    out[:rows, span] = jnp.round(parts).astype(jnp.int32).astype(jnp.int16)
    tail = jnp.zeros((out.shape[0] - rows, LANES), jnp.float32)
    for i in range(0, rows, LANES):
        some = log[i : i + LANES]
        there = iota((some.shape[0], LANES), 0) == iota((some.shape[0], LANES), 1)
        line = jnp.sum(jnp.where(there, some, 0.0), axis=0, keepdims=True)
        tail = jnp.where(iota(tail.shape, 0) == i // LANES, line, tail)
    out[rows:, span] = tail.astype(jnp.int32).astype(jnp.int16)


def decoded(code, column, rows):
    span = slice(column * LANES, (column + 1) * LANES)
    tail = code[rows:, span].astype(jnp.int32).astype(jnp.float32)
    logs = []
    for i in range(0, rows, LANES):
        count = min(LANES, rows - i)
        there = iota((count, LANES), 0) == iota((count, LANES), 1)
        line = tail[i // LANES : i // LANES + 1]
        logs.append(jnp.sum(jnp.where(there, line, 0.0), axis=1, keepdims=True))
    scale = jnp.exp2(jnp.concatenate(logs, axis=0) * (1.0 / STEPS)) * (1.0 / TOP)
    return code[:rows, span].astype(jnp.int32).astype(jnp.float32) * scale


BLOCK = 2 * GROUP


def laid(chunks, held):
    row = 0
    for chunk in chunks:
        held[row : row + chunk.shape[0]] = chunk[...]
        row += chunk.shape[0]


def soon_kernel(count, pick, *refs):
    chunks, before, outs, held = refs[:count], refs[count:-3], refs[-3:-1], refs[-1]
    laid(chunks, held)
    half = outs[0].shape[0]
    for k, out in enumerate(outs):
        for row in range(0, half, BLOCK):
            span, of = slice(row, row + BLOCK), slice(k * half + row, k * half + row + BLOCK)
            rows = jnp.dot(pick[of], held[...], preferred_element_type=jnp.float32)
            if before:
                rows += before[k][span].astype(jnp.float32)
            out[span] = rows.astype(jnp.bfloat16)


def soon(pick, chunks, before=()):
    rows, depth = pick.shape
    width = chunks[0].shape[1]
    return pl.pallas_call(
        functools.partial(soon_kernel, len(chunks)),
        out_shape=(jax.ShapeDtypeStruct((rows // 2, width), jnp.bfloat16),) * 2,
        in_specs=[VMEM] * (1 + len(chunks) + len(before)),
        out_specs=(VMEM,) * 2,
        scratch_shapes=[pltpu.VMEM((depth, width), jnp.bfloat16)],
        compiler_params=pltpu.CompilerParams(vmem_limit_bytes=14 << 20),
        cost_estimate=pl.CostEstimate(
            flops=2 * rows * depth * width, bytes_accessed=1 << 23, transcendentals=0
        ),
    )(pick, *chunks, *before)


def joined(early, pick, late, out):
    for row in range(0, out.shape[0], BLOCK):
        span = slice(row, row + BLOCK)
        rows = jnp.dot(pick[span], late[...], preferred_element_type=jnp.float32)
        out[span] = (rows + early[span].astype(jnp.float32)).astype(jnp.bfloat16)


def piece_sums(xs, span, pieces):
    x = jnp.concatenate([x[span] for x in xs], axis=1)
    w = jnp.concatenate([jnp.concatenate([w[0], w[1]], axis=1) for w in pieces], axis=0)
    return jnp.dot(x, w, preferred_element_type=jnp.float32)


GIVE, KEEP = slice(2 * GROUP, 4 * GROUP), slice(0, 2 * GROUP)


def coded_pair(sums, outs, j):
    for k in range(2):
        for i in range(2):
            some = sums[k * GROUP : (k + 1) * GROUP, i * LANES : (i + 1) * LANES]
            coded(some, outs[k], 2 * j + i)


def begin_kernel(early, pick, first, second, *refs):
    pieces, xa, begun, late = refs[:-3], refs[-3], refs[-2], refs[-1]
    laid((first, second), late)
    joined(early, pick, late, xa)
    for j, near in enumerate(pieces):
        begun[:, 2 * j * LANES : 2 * (j + 1) * LANES] = piece_sums((xa,), GIVE, (near,))


def begin(early, pick, last, near):
    width = len(near) * 2 * LANES
    late = sum(part.shape[0] for part in last)
    return pl.pallas_call(
        begin_kernel,
        out_shape=(
            jax.ShapeDtypeStruct(early.shape, jnp.bfloat16),
            jax.ShapeDtypeStruct((2 * GROUP, width), jnp.float32),
        ),
        in_specs=[VMEM] * (4 + len(near)),
        out_specs=(VMEM,) * 2,
        scratch_shapes=[pltpu.VMEM((late, early.shape[1]), jnp.bfloat16)],
        compiler_params=pltpu.CompilerParams(vmem_limit_bytes=12 << 20),
        cost_estimate=pl.CostEstimate(
            flops=4 * GROUP * early.shape[1] * width, bytes_accessed=1 << 22, transcendentals=0
        ),
    )(early, pick, *last, *near)


def end_kernel(begun, early, pick, first, second, *refs):
    pieces, xb, outs, late = refs[:-4], refs[-4], refs[-3:-1], refs[-1]
    laid((first, second), late)
    joined(early, pick, late, xb)
    for j, far in enumerate(pieces):
        sums = piece_sums((xb,), GIVE, (far,))
        coded_pair(sums + begun[:, 2 * j * LANES : 2 * (j + 1) * LANES], outs, j)


def end(begun, early, pick, last, far):
    late = sum(part.shape[0] for part in last)
    width = len(far) * 2 * LANES
    return pl.pallas_call(
        end_kernel,
        out_shape=(
            jax.ShapeDtypeStruct(early.shape, jnp.bfloat16),
            *(jax.ShapeDtypeStruct((GROUP + 8, width), jnp.int16),) * 2,
        ),
        in_specs=[VMEM] * (5 + len(far)),
        out_specs=(VMEM,) * 3,
        scratch_shapes=[pltpu.VMEM((late, early.shape[1]), jnp.bfloat16)],
        compiler_params=pltpu.CompilerParams(vmem_limit_bytes=12 << 20),
        cost_estimate=pl.CostEstimate(
            flops=4 * GROUP * early.shape[1] * width, bytes_accessed=1 << 22, transcendentals=0
        ),
    )(begun, early, pick, *last, *far)


def give_kernel(xa, xb, *refs):
    count = (len(refs) - 2) // 2
    for j in range(count):
        coded_pair(piece_sums((xa, xb), GIVE, (refs[j], refs[count + j])), refs[-2:], j)


def keep_kernel(xa, xb, *refs):
    count = (len(refs) - 2) // 2
    for j in range(count):
        sums = piece_sums((xa, xb), KEEP, (refs[j], refs[count + j]))
        for k in range(2):
            refs[2 * count + k][:, 2 * j * LANES : 2 * (j + 1) * LANES] = sums[
                k * GROUP : (k + 1) * GROUP
            ]


def product(kernel, xs, pieces, width, rows, kind):
    depth = 2 * xs[1].shape[1]
    return pl.pallas_call(
        kernel,
        out_shape=(jax.ShapeDtypeStruct((rows, width), kind),) * 2,
        in_specs=[VMEM] * (len(xs) + len(pieces)),
        out_specs=(VMEM,) * 2,
        compiler_params=pltpu.CompilerParams(vmem_limit_bytes=14 << 20),
        cost_estimate=pl.CostEstimate(
            flops=4 * GROUP * depth * width,
            bytes_accessed=8 * GROUP * width + 2 * depth * (2 * GROUP + width),
            transcendentals=0,
        ),
    )(*xs, *pieces)


def gated_kernel(first, here, *refs):
    keeps, codes, out = refs[:2], refs[2:4], refs[-1]
    rows = keeps[0].shape[0]
    y, core = here[1], here[4]
    for j in range(2):
        o = first + j
        piece = (y + (0, SETS - 1, 1, 2)[o]) & (SETS - 1)
        pad = jnp.zeros((DEAL_PAD - DEAL, LANES), jnp.float32)
        for k in range(2):
            gate, up = (
                keeps[k][:, (2 * o + i) * LANES : (2 * o + i + 1) * LANES]
                + decoded(codes[k], 2 * j + i, rows)
                for i in range(2)
            )
            hidden = gate / (1.0 + jnp.exp(-gate)) * up
            for c in range(HALVES * SETS):
                some = jnp.concatenate([hidden[c * DEAL : (c + 1) * DEAL], pad], axis=0)
                out[c, k ^ core, piece] = some.astype(jnp.bfloat16)


def placed_kernel(got, places, out):
    for e in range(2):
        for h in range(HALVES):
            lines = [
                jnp.concatenate([got[h * SETS + s, e, p] for p in range(SETS)], axis=1)
                for s in range(SETS)
            ]
            rows = jnp.concatenate(lines, axis=0)
            wide = rows.shape[1]
            out[e, :, h * wide : (h + 1) * wide] = jnp.dot(
                places[e], rows, preferred_element_type=jnp.float32
            ).astype(jnp.bfloat16)


def shards(tokens, expert_ids, w_gate, w_up):
    z = lax.axis_index("z")
    y = lax.axis_index("y")
    x_lo = lax.axis_index("x_lo")
    x_hi = lax.axis_index("x_hi")
    core = lax.axis_index("core")
    near, far = weights_of_ring(w_gate, w_up, core)

    blocks = expert_ids.shape[0] // LANES
    low = ((x_lo * SETS + y) * QUARTERS + 2 * x_hi + core) * SLOTS_DEV
    here = jnp.stack([z, y, low, 2 * x_hi + core, core]).astype(jnp.int32)
    chunk, code, rank, own, at = pl.pallas_call(
        deal_kernel,
        out_shape=(
            jax.ShapeDtypeStruct((SEND, tokens.shape[1]), jnp.bfloat16),
            jax.ShapeDtypeStruct((blocks, LANES), jnp.int32),
            jax.ShapeDtypeStruct((3, blocks, LANES), jnp.int32),
            jax.ShapeDtypeStruct((blocks, LANES), jnp.int32),
            jax.ShapeDtypeStruct((ROWS, 8, LANES), jnp.int32),
        ),
        in_specs=[VMEM, pl.BlockSpec(memory_space=pl.ANY)],
        out_specs=(VMEM,) * 5,
        scratch_shapes=[
            pltpu.VMEM(tokens.shape, jnp.bfloat16),
            pltpu.SemaphoreType.DMA((COPIES,)),
        ],
        compiler_params=pltpu.CompilerParams(vmem_limit_bytes=60 << 20),
        cost_estimate=pl.CostEstimate(flops=1 << 30, bytes_accessed=1 << 22, transcendentals=0),
    )(expert_ids.T, tokens)
    chunks, last = rows_of_ring(chunk)

    moved, places = pl.pallas_call(
        lists_kernel,
        out_shape=(
            jax.ShapeDtypeStruct((ROWS, 8, SEND), jnp.float32),
            jax.ShapeDtypeStruct((2, SLOTS_DEV, SETS * DEAL_PAD), jnp.bfloat16),
        ),
        in_specs=[SMEM] + [VMEM] * 4,
        out_specs=(VMEM,) * 2,
        compiler_params=pltpu.CompilerParams(vmem_limit_bytes=8 << 20),
        cost_estimate=pl.CostEstimate(flops=1 << 30, bytes_accessed=1 << 20, transcendentals=0),
    )(here, code, rank, own, at)
    moved = moved.astype(jnp.int32)
    rows = jnp.arange(QUARTERS * GROUP)
    pick, other = (
        (rows[:, None] + 1 == (moved[:, 2 * i] * 32 + moved[:, 2 * i + 1]).reshape(1, -1)).astype(
            jnp.bfloat16
        )
        for i in range(2)
    )

    both = jnp.concatenate([pick, other])
    own, give = soon(both[:, : 5 * SEND], chunks[:5])
    own, give = soon(both[:, 5 * SEND : 7 * SEND], chunks[5:], (own, give))
    early_b = lax.ppermute(give, "core", SWAP)
    last_b = [lax.ppermute(part, "core", SWAP) for part in last]
    late = pick[:, 7 * SEND :]
    width = 4 * LANES
    xa, begun = begin(own, late, last, near[:2])
    xb, *first = end(begun, early_b, late, last_b, far[:2])
    xs = (xa, xb)
    gives = [
        lambda: first,
        lambda: product(give_kernel, xs, near[2:] + far[2:], width, GROUP + 8, jnp.int16),
    ]
    gots = []
    for give in gives:
        same, cross = give()
        gots.append(lax.ppermute(same, "x_hi", SWAP))
        gots.append(lax.ppermute(cross, ("x_hi", "core"), [(i, 3 - i) for i in range(4)]))
    same, cross = product(keep_kernel, xs, near + far, 2 * width, GROUP, jnp.float32)
    cross = lax.ppermute(cross, "core", SWAP)
    hidden = ()
    for part in range(2):
        hidden = pl.pallas_call(
            functools.partial(gated_kernel, 2 * part),
            out_shape=jax.ShapeDtypeStruct((HALVES * SETS, 2, SETS, DEAL_PAD, LANES), jnp.bfloat16),
            in_specs=[SMEM] + [VMEM] * (4 + len(hidden)),
            out_specs=VMEM,
            input_output_aliases={5: 0} if hidden else {},
            compiler_params=pltpu.CompilerParams(vmem_limit_bytes=8 << 20),
            cost_estimate=pl.CostEstimate(flops=1 << 29, bytes_accessed=1 << 21, transcendentals=0),
        )(here, same, cross, *gots[2 * part : 2 * part + 2], *hidden)
        hidden = (hidden,)
    hidden = hidden[0]
    hidden = lax.all_to_all(hidden, ("x_lo", "y"), 0, 0)
    return pl.pallas_call(
        placed_kernel,
        out_shape=jax.ShapeDtypeStruct((2, SLOTS_DEV, HALVES * SETS * LANES), jnp.bfloat16),
        in_specs=[VMEM] * 2,
        out_specs=VMEM,
        compiler_params=pltpu.CompilerParams(vmem_limit_bytes=8 << 20),
        cost_estimate=pl.CostEstimate(flops=1 << 28, bytes_accessed=1 << 20, transcendentals=0),
    )(hidden, places)


def solution(mesh):
    cut = jax.sharding.Mesh(
        mesh.devices.reshape(ROWS, HALVES, SETS, 2, 2), ("z", "x_lo", "y", "x_hi", "core")
    )
    layer, col = ("x_hi", "core"), ("x_lo", "y")
    in_specs = (P("z", layer), P(), P(None, layer, ("z", *col)), P(None, layer, ("z", *col)))
    out_specs = P(None, (*col, *layer), "z")
    return jax.shard_map(shards, mesh=cut, in_specs=in_specs, out_specs=out_specs, check_vma=False)
```
